32 devices in a mesh: inst: 4 (over x, core), shard: 8 (over z, y).
Axes of the slice: x: 2, y: 2, z: 4, core: 2. Of those that a mesh axis runs over, the one named last changes fastest.
Arguments:
- tokens: bfloat16 [2048, 5120], P(('inst', 'shard')), may hold values from -600 to 600
- norm_gain: float32 [5120], P(('inst', 'shard')), may hold values from 0.1 to 1.9
- master_qkv: float32 [5120, 7168], P(('inst', 'shard')), may hold values from -0.078125 to 0.078125
- qkv_bias: float32 [7168], P(('inst', 'shard')), may hold values from -3 to 3
Outputs:
- qkv_out: bfloat16 [32, 512, 896], P(('inst', 'shard'))
The draws below stay inside these ranges and needn't reach their ends.
All inputs are finite; a program needn't handle non-finite values.
Results may differ from the reference program's by a relative error of at most 0.0062.
Values may be sent and summed in bfloat16 or wider, within the bound.
No kernel may reach another device: no remote copies, remote signals or barrier semaphores. Data moves between devices by JAX's collectives and lax.ppermute only.
A program may use at most 64 MiB of HBM per device.

```python
import jax
import jax.numpy as jnp
from jax import lax

D = 5120
QHEADS = 40
KVHEADS = 8
HEAD_DIM = 128
TP = 8
TOK_DEV = 64
QKVW = 7168
TOKENS = 2048
N_INST = 4
N_SHARD = 8


def draw_tokens(key, part):
    row_key, col_key, base_key = jax.random.split(key, 3)
    base = jax.random.truncated_normal(base_key, -4.0, 4.0, (TOKENS, D), jnp.float32)
    row_scale = jnp.power(10.0, jax.random.uniform(row_key, (TOKENS, 1), jnp.float32, 0.0, 1.0))
    col_scale = jnp.power(10.0, jax.random.uniform(col_key, (1, D), jnp.float32, 0.0, 1.0))
    return (base * row_scale * col_scale).astype(jnp.bfloat16)


def block_scale(stream_key, shape, cuts, smallest, largest):
    level = 1.0
    for position, shards_of in cuts:
        heights = jax.random.uniform(jax.random.fold_in(jax.random.fold_in(stream_key, 6), position), (shards_of,), jnp.float32, smallest / len(cuts), largest / len(cuts))
        level = level * jnp.repeat(jnp.exp(heights), shape[position] // shards_of).reshape((-1,) + (1,) * (len(shape) - 1 - position))
    return level


def scatter_about(stream_key, extent, scale, bound, cuts=(), dtype=jnp.bfloat16):
    entries = jax.random.normal(stream_key, extent, jnp.float32) * scale
    if len(cuts) > 0:
        entries = block_scale(stream_key, extent, cuts, -0.22, 0.18) * entries
    return jnp.clip(entries, min=-bound, max=bound).astype(dtype)


def setup_inputs(seed: int = 0) -> dict:
    key_of = jax.random.split(jax.random.key(seed), 5)
    tokens = draw_tokens(jax.random.fold_in(key_of[4], 71), 0)
    norm_gain = jnp.clip(1.0 + 0.18 * jax.random.normal(key_of[1], (D,), jnp.float32), 0.1, 1.9)
    master_qkv = scatter_about(key_of[2], (D, QKVW), D ** -0.5, 0.078125, ((0, 32),), jnp.float32)
    qkv_bias = scatter_about(key_of[3], (QKVW,), 0.5, 3.0, ((0, 32),), jnp.float32)
    return {"tokens": tokens, "norm_gain": norm_gain, "master_qkv": master_qkv, "qkv_bias": qkv_bias}


EPSILON = 1e-06

def rank_columns(matrix):
    query_cols = QHEADS * HEAD_DIM
    pair_cols = KVHEADS * HEAD_DIM
    leading = matrix.shape[:-1]
    query = matrix[..., :query_cols].reshape(leading + (TP, query_cols // TP))
    keys = matrix[..., query_cols:query_cols + pair_cols].reshape(leading + (TP, pair_cols // TP))
    values = matrix[..., query_cols + pair_cols:].reshape(leading + (TP, pair_cols // TP))
    return jnp.concatenate([query, keys, values], axis=-1)

def normalize(tokens, gain):
    floats = tokens.astype(jnp.float32)
    scale = lax.rsqrt(lax.optimization_barrier(jnp.mean(floats * floats, axis=-1, keepdims=True)) + EPSILON)
    return (floats * scale * gain.astype(jnp.float32)).astype(jnp.bfloat16)

def reference(tokens, norm_gain, master_qkv, qkv_bias):
    weights = master_qkv.astype(jnp.bfloat16)
    gain_low = norm_gain.astype(jnp.bfloat16)
    bias_low = qkv_bias.astype(jnp.bfloat16)
    normed = normalize(tokens, gain_low)
    rank_width = QKVW // TP
    flat_weights = rank_columns(weights).reshape(D, TP * rank_width)
    flat_bias = rank_columns(bias_low).reshape(TP * rank_width).astype(jnp.float32)
    group_tokens = TP * TOK_DEV
    groups = normed.reshape(TOKENS // group_tokens, group_tokens, D)

    def project(group_rows):
        product = jnp.dot(group_rows, flat_weights, preferred_element_type=jnp.float32) + flat_bias
        shaped = product.astype(jnp.bfloat16).reshape(group_tokens, TP, rank_width)
        return jnp.transpose(shaped, (1, 0, 2))
    outputs = lax.map(project, groups)
    return outputs.reshape(N_INST * N_SHARD, group_tokens, rank_width)
```

```python
import functools

import jax
import jax.numpy as jnp
from jax import lax
from jax.experimental import pallas as pl
from jax.experimental.pallas import tpu as pltpu
from jax.sharding import PartitionSpec as P

QHEADS = 40
KVHEADS = 8
HEAD_DIM = 128
TP = 8
QUERY_COLS = QHEADS * HEAD_DIM
PAIR_COLS = KVHEADS * HEAD_DIM

EPSILON = 1e-06

QUAD = TP // 2
LOW = 4
VMEM = pl.BlockSpec(memory_space=pltpu.VMEM)
ANY = pl.BlockSpec(memory_space=pl.ANY)


def exchange(value, axis, mask):
    pairs = [(source, source ^ mask) for source in range(lax.axis_size(axis))]
    return lax.ppermute(value, axis, pairs)


def bit_of(index, position):
    return jnp.bitwise_and(jnp.right_shift(index, position), 1)


def ordered(mine, theirs, upper):
    return jnp.where(
        upper == 0, jnp.concatenate([mine, theirs], 0), jnp.concatenate([theirs, mine], 0)
    )


def bits_of(count):
    return range(count.bit_length() - 1)


def place():
    rank = lax.rem(lax.axis_index("shard"), TP)
    return lax.div(rank, QUAD), lax.rem(rank, QUAD)


def bf16_shapes(shapes):
    return [jax.ShapeDtypeStruct(shape, jnp.bfloat16) for shape in shapes]


def token_body(tokens_ref, keep_ref, give_ref):
    half, _ = place()
    low = lax.rem(lax.axis_index("inst"), LOW)
    width = tokens_ref.shape[1] // (2 * LOW)
    floats = tokens_ref[...].astype(jnp.float32)
    scale = lax.rsqrt(jnp.mean(floats * floats, axis=-1, keepdims=True) + EPSILON)
    for out_ref, part in ((keep_ref, half), (give_ref, 1 - half)):
        for mask in range(LOW):
            start = (jnp.bitwise_xor(low, mask) * 2 + part) * width
            block = tokens_ref[:, pl.ds(pl.multiple_of(start, 128), width)].astype(jnp.float32)
            out_ref[:, mask * width : (mask + 1) * width] = (block * scale).astype(jnp.bfloat16)


def prepare_tokens(tokens):
    count, features = tokens.shape
    return pl.pallas_call(
        token_body,
        out_shape=bf16_shapes([(count, features // 2)] * 2),
        in_specs=[VMEM],
        out_specs=[VMEM] * 2,
    )(tokens)


def weight_body(other, cuts, gain_ref, master_ref, *refs):
    out_refs, (scratch, sems) = refs[:-2], refs[-2:]
    half, quad_pos = place()
    part = 1 - half if other else half
    spans = ((0, QUERY_COLS // TP), (QUERY_COLS, PAIR_COLS // TP), (QUERY_COLS + PAIR_COLS, PAIR_COLS // TP))
    copies = []
    for mask in range(QUAD):
        rank = part * QUAD + jnp.bitwise_xor(quad_pos, mask)
        offset = 0
        for number, (first, width) in enumerate(spans):
            start = pl.multiple_of(first + rank * width, 128)
            copies.append(
                pltpu.make_async_copy(
                    master_ref.at[:, pl.ds(start, width)],
                    scratch.at[mask, :, pl.ds(offset, width)],
                    sems.at[mask, number],
                )
            )
            offset += width
    for copy in copies:
        copy.start()
    gain = gain_ref[...].astype(jnp.bfloat16).astype(jnp.float32)
    for mask in range(QUAD):
        for number in range(len(spans)):
            copies[mask * len(spans) + number].wait()
        for chunk, (start, stop) in enumerate(cuts):
            block = scratch[mask, :, start:stop].astype(jnp.bfloat16).astype(jnp.float32)
            out_refs[chunk * QUAD + mask][...] = (block * gain).astype(jnp.bfloat16)


def prepare_weights(gain, master, other, cuts):
    rows, width = master.shape
    outs = pl.pallas_call(
        functools.partial(weight_body, other, cuts),
        out_shape=bf16_shapes([(rows, stop - start) for start, stop in cuts for _ in range(QUAD)]),
        in_specs=[VMEM, ANY],
        out_specs=[VMEM] * (QUAD * len(cuts)),
        scratch_shapes=[
            pltpu.VMEM((QUAD, rows, width // TP), jnp.float32),
            pltpu.SemaphoreType.DMA((QUAD, 3)),
        ],
    )(gain, master)
    return [outs[chunk * QUAD : (chunk + 1) * QUAD] for chunk in range(len(cuts))]


def assemble_body(*refs):
    out_ref = refs[-1]
    _, quad_pos = place()
    rows = refs[0].shape[0]
    for mask in range(QUAD):
        start = pl.multiple_of(jnp.bitwise_xor(quad_pos, mask) * rows, 16)
        out_ref[pl.ds(start, rows), :] = refs[mask][...]


def assemble(pieces):
    rows, width = pieces[0].shape
    if rows % 16 == 0:
        return pl.pallas_call(
            assemble_body,
            out_shape=bf16_shapes([(QUAD * rows, width)])[0],
            in_specs=[VMEM] * QUAD,
            out_specs=VMEM,
        )(*pieces)
    _, quad_pos = place()
    step = 1
    while step < QUAD:
        swap = jnp.bitwise_and(quad_pos, step) != 0
        pieces = [jnp.where(swap, pieces[at ^ step], pieces[at]) for at in range(QUAD)]
        step *= 2
    return jnp.concatenate(pieces, 0)


def spread_rows(pieces):
    shard_pos, instance = lax.axis_index("shard"), lax.axis_index("inst")
    block = assemble(
        [pieces[0]] + [exchange(pieces[mask], "shard", mask) for mask in range(1, QUAD)]
    )
    for position in bits_of(lax.axis_size("shard") // TP):
        theirs = exchange(block, "shard", TP << position)
        block = ordered(block, theirs, bit_of(shard_pos, position + TP.bit_length() - 1))
    for position in bits_of(lax.axis_size("inst") // LOW):
        theirs = exchange(block, "inst", LOW << position)
        block = ordered(block, theirs, bit_of(instance, position + LOW.bit_length() - 1))
    across = exchange(block, "inst", 2)
    return [block, exchange(block, "inst", 1), across, exchange(across, "inst", 1)]


def matmul_body(*refs):
    token_refs, weight_refs = refs[:TP], refs[TP : TP + LOW]
    out_ref, rows_ref = refs[TP + LOW :]
    count = token_refs[0].shape[0]

    @pl.when(pl.program_id(0) == 0)
    def _():
        for number, token_ref in enumerate(token_refs):
            rows_ref[number * count : (number + 1) * count, :] = token_ref[...]

    depth = weight_refs[0].shape[0]
    total = None
    for number, weight_ref in enumerate(weight_refs):
        term = jnp.dot(
            rows_ref[:, number * depth : (number + 1) * depth],
            weight_ref[...],
            preferred_element_type=jnp.float32,
        )
        total = term if total is None else total + term
    out_ref[...] = total.astype(out_ref.dtype)


def matmul(token_pieces, blocks, dtype):
    count, features = token_pieces[0].shape
    depth, width = blocks[0].shape
    tile = 256 if width % 256 == 0 else 128
    rows = TP * count
    return pl.pallas_call(
        matmul_body,
        grid=(width // tile,),
        out_shape=jax.ShapeDtypeStruct((rows, width), dtype),
        in_specs=[pl.BlockSpec((count, features), lambda step: (0, 0))] * TP
        + [pl.BlockSpec((depth, tile), lambda step: (0, step))] * LOW,
        out_specs=pl.BlockSpec((rows, tile), lambda step: (0, step)),
        scratch_shapes=[pltpu.VMEM((rows, features), jnp.bfloat16)],
        cost_estimate=pl.CostEstimate(
            flops=2 * rows * features * width,
            bytes_accessed=2 * (rows * features + features * width + rows * width),
            transcendentals=0,
        ),
    )(*token_pieces, *blocks)


def finish_body(*refs):
    mine_ref, bias_ref, out_ref = refs[0], refs[1], refs[-1]
    half, quad_pos = place()
    rank = half * QUAD + quad_pos
    count = mine_ref.shape[0] // TP
    spans = ((0, QUERY_COLS // TP), (QUERY_COLS, PAIR_COLS // TP), (QUERY_COLS + PAIR_COLS, PAIR_COLS // TP))
    bias = jnp.concatenate(
        [
            bias_ref[:, pl.ds(pl.multiple_of(first + rank * width, 128), width)]
            for first, width in spans
        ],
        axis=1,
    ).astype(jnp.float32)
    for number in range(TP):
        rows = slice(number * count, (number + 1) * count)
        crossed = slice((number ^ QUAD) * count, ((number ^ QUAD) + 1) * count)
        place_out = pl.multiple_of(jnp.bitwise_xor(rank, number) * count, count)
        start = 0
        for part_ref in refs[2:-1]:
            stop = start + part_ref.shape[1]
            value = mine_ref[rows, start:stop] + part_ref[crossed, :].astype(jnp.float32)
            out_ref[0, pl.ds(place_out, count), start:stop] = (
                value + bias[:, start:stop]
            ).astype(jnp.bfloat16)
            start = stop


def finish(mine, bias, parts):
    return pl.pallas_call(
        finish_body,
        out_shape=jax.ShapeDtypeStruct((1,) + mine.shape, jnp.bfloat16),
        in_specs=[VMEM] * (2 + len(parts)),
        out_specs=VMEM,
    )(mine, bias, *parts)


def gather_bias(bias):
    rows = bias.astype(jnp.bfloat16).astype(jnp.float32).reshape(1, -1)
    shards, instances = lax.axis_size("shard"), lax.axis_size("inst")
    index = lax.axis_index("inst") * shards + lax.axis_index("shard")
    for position in bits_of(shards):
        rows = jnp.concatenate([rows, exchange(rows, "shard", 1 << position)], 0)
    for position in bits_of(instances):
        rows = jnp.concatenate([rows, exchange(rows, "inst", 1 << position)], 0)
    order = jnp.bitwise_xor(jnp.arange(shards * instances), index)
    return rows[order].reshape(1, -1)


def gather_quad(piece):
    along = exchange(piece, "shard", 2)
    return [piece, exchange(piece, "shard", 1), along, exchange(along, "shard", 1)]


def per_device(tokens, norm_gain, master_qkv, qkv_bias):
    instances = lax.axis_size("inst")
    copies = lax.axis_size("shard") // TP
    local_rows = master_qkv.shape[0]
    rank_width = master_qkv.shape[1] // TP
    count, features = tokens.shape

    if instances * copies > LOW:
        tokens = tokens.reshape(count, instances // LOW, LOW, copies, 2, QUAD * local_rows)
        tokens = jnp.transpose(tokens, (0, 2, 4, 1, 3, 5)).reshape(count, features)
    keep, give = prepare_tokens(tokens)
    got = exchange(give, "shard", QUAD)
    group = gather_quad(keep) + gather_quad(got)

    cut = (rank_width // 2 + HEAD_DIM - 1) // HEAD_DIM * HEAD_DIM
    gain = norm_gain[:, None]
    theirs = prepare_weights(gain, master_qkv, True, ((0, cut), (cut, rank_width)))
    mine = prepare_weights(gain, master_qkv, False, ((0, rank_width),))

    parts = []
    for pieces in theirs:
        partial = matmul(group, spread_rows(pieces), jnp.bfloat16)
        parts.append(exchange(partial, "shard", QUAD))
    own = matmul(group, spread_rows(mine[0]), jnp.float32)
    return finish(own, gather_bias(qkv_bias), parts)


def solution(mesh):
    in_specs = (
        P(("inst", "shard"), None),
        P(("inst", "shard")),
        P(("inst", "shard"), None),
        P(("inst", "shard")),
    )
    out_specs = P(("inst", "shard"), None, None)
    return jax.shard_map(
        per_device, mesh=mesh, in_specs=in_specs, out_specs=out_specs, check_vma=False
    )
```
